512 devices in a mesh: dp: 32 (over x, z), patch: 16 (over y, core).
Axes of the slice: x: 4, y: 8, z: 8, core: 2. Of those that a mesh axis runs over, the one named last changes fastest.
Arguments:
- query_rows: bfloat16 [32, 2048, 576], P('dp', 'patch'), may hold values from -6 to 6
- key_rows: bfloat16 [32, 2048, 576], P('dp', 'patch'), may hold values from -6 to 6
- value_rows: bfloat16 [32, 2048, 576], P('dp', 'patch'), may hold values from -6 to 6
- out_weight: bfloat16 [576, 1152], replicated, may hold values from -0.25 to 0.25
- target: bfloat16 [32, 2048, 1152], P('dp', 'patch'), may hold values from -6 to 6
- lengths: int32 [32], P('dp'), may hold values from 256 to 2048
- segments: int32 [32, 2048], P('dp', 'patch'), may hold values from 0 to 7, never falling along the last dimension, each value on 1 to 1024 neighbouring positions
Outputs:
- query_grad: float32 [32, 2048, 576], P('dp', 'patch')
- key_grad: float32 [32, 2048, 576], P('dp', 'patch')
- value_grad: float32 [32, 2048, 576], P('dp', 'patch')
- weight_grad: float32 [576, 1152], P('patch', 'dp')
- loss: float32 [], replicated
The draws below stay inside these ranges and needn't reach their ends.
All inputs are finite; a program needn't handle non-finite values.
Results may differ from the reference program's by a relative error of at most 0.024.
Values may be sent and summed in bfloat16 or wider, within the bound.
A program may use at most 64 MiB of HBM per device.

```python
import math
import jax
import jax.numpy as jnp
import numpy as np
from jax import lax

WIDTH = 1152
HEADS = 8
HEAD_DIM = 72
TOK_DEV = 128
FEAT = 576
SEQ = 2048
SAMPLES = 32


def draw_rows(key, salt, chosen_rows):
    fresh_key = jax.random.fold_in(key, salt)
    sampled = jnp.clip(1.5 * jax.random.normal(fresh_key, (SAMPLES, SEQ, FEAT), jnp.float32), -6.0, 6.0)
    return sampled.astype(jnp.bfloat16)


def draw_query_rows(key, part):
    positions = jnp.arange(SEQ)
    return draw_rows(key, 1, positions % TOK_DEV == 0)


def draw_key_rows(key, part):
    positions = jnp.arange(SEQ)
    return draw_rows(key, 2, positions % TOK_DEV == 0)


def plant(entries, key, low, largest):
    longest = entries.shape.index(max(entries.shape))
    spots = []
    for shift in (0, 1):
        where = [jax.random.randint(jax.random.fold_in(key, axis), (), 0, length) for axis, length in enumerate(entries.shape)]
        where[longest] = (where[longest] + shift) % entries.shape[longest]
        spots.append(tuple(where))
    return entries.at[spots[0]].set(low).at[spots[1]].set(largest)


def steps_of(stream_key, extent, split, least, largest):
    level = 1.0
    for position, shards_of in split:
        heights = jax.random.uniform(jax.random.fold_in(jax.random.fold_in(stream_key, 6), position), (shards_of,), jnp.float32, least / len(split), largest / len(split))
        level = level * jnp.repeat(jnp.exp(heights), extent[position] // shards_of).reshape((-1,) + (1,) * (len(extent) - 1 - position))
    return level


def profile(count, total, most, skew):
    weights = [(1 << 20) // math.isqrt(rank ** skew) + 1 for rank in range(2, count + 1)]
    surplus, counts = total - most - (count - 1), [1] * (count - 1)
    while surplus > 0:
        candidates = [i for i in range(count - 1) if counts[i] < most]
        pool, remaining = sum([weights[i] for i in candidates]), surplus
        for i in candidates:
            more = min(most - counts[i], max(1, remaining * weights[i] // pool), surplus)
            counts[i] = counts[i] + more
            surplus = surplus - more
    return np.array([most] + counts)


def uneven_parts(key, number_of, total, most, skew):
    if number_of == 2:
        one = jax.random.randint(key, (), max(1, total - most), min(most, total - 1) + 1)
        return jnp.stack([one, total - one])
    tallies = jnp.asarray(profile(number_of, total, most, skew), jnp.int32)
    pairs = (number_of - 1) // 2
    donor, sink = tallies[1:1 + 2 * pairs:2], tallies[2:2 + 2 * pairs:2]
    slack = jnp.minimum(donor - 1, most - sink)
    shifted = jax.random.randint(jax.random.fold_in(key, 1), (pairs,), 0, 1 << 20) % (slack + 1)
    tallies = tallies.at[1:1 + 2 * pairs:2].set(donor - shifted).at[2:2 + 2 * pairs:2].set(sink + shifted)
    return tallies[jax.random.permutation(jax.random.fold_in(key, 2), number_of)]


def normal_values(rng, shape, spread, most, split=(), kind=jnp.bfloat16):
    array = spread * jax.random.normal(rng, shape, jnp.float32)
    if split:
        array = array * steps_of(rng, shape, split, -0.22, 0.18)
    return jnp.clip(array, -most, most).astype(kind)


def setup_inputs(seed: int = 0) -> dict:
    arg_keys = jax.random.split(jax.random.key(seed), 8)
    query_rows = draw_query_rows(jax.random.fold_in(arg_keys[7], 71), 0)
    key_rows = draw_key_rows(jax.random.fold_in(arg_keys[7], 71), 0)
    value_rows = normal_values(arg_keys[2], (SAMPLES, SEQ, FEAT), 1.0, 6.0, ((0, 32), (1, 16)))
    out_weight = normal_values(arg_keys[3], (FEAT, WIDTH), FEAT ** -0.5, 0.25)
    target = normal_values(arg_keys[4], (SAMPLES, SEQ, WIDTH), 1.0, 6.0, ((0, 32), (1, 16)))
    lengths = plant(jax.random.randint(arg_keys[5], (SAMPLES,), SEQ // 8, SEQ + 1), jax.random.fold_in(arg_keys[5], 1), SEQ // 8, SEQ).astype(jnp.int32)
    segments = jax.vmap(lambda own: jnp.searchsorted(jnp.cumsum(uneven_parts(own, 8, SEQ, SEQ // 2, 2)), jnp.arange(SEQ), side="right"))(jax.random.split(arg_keys[6], SAMPLES)).reshape((SAMPLES, SEQ)).astype(jnp.int32)
    return {"query_rows": query_rows, "key_rows": key_rows, "value_rows": value_rows, "out_weight": out_weight, "target": target, "lengths": lengths, "segments": segments}


NEG_LARGE = -1e+30

def widen(value):
    return lax.optimization_barrier(value).astype(jnp.float32)

def one_sample(packed, out_weight):
    query_rows, key_rows, value_rows, target_rows, length, segment_row = packed
    score_scale = 1.0 / math.sqrt(HEAD_DIM)
    query_heads = query_rows.astype(jnp.float32).reshape(SEQ, HEADS, HEAD_DIM)
    key_heads = key_rows.astype(jnp.float32).reshape(SEQ, HEADS, HEAD_DIM)
    value_heads = value_rows.astype(jnp.float32).reshape(SEQ, HEADS, HEAD_DIM)
    live = lax.iota(jnp.int32, SEQ) < length
    group = jnp.where(live, segment_row, -1)
    allowed = (group[:, None] == group[None, :])[None, :, :]
    scores = jnp.einsum('qhe,khe->hqk', query_heads, key_heads) * score_scale
    masked = jnp.where(allowed, scores, NEG_LARGE)
    row_max = lax.optimization_barrier(jnp.max(masked, axis=2))
    probs = jnp.where(allowed, jnp.exp(masked - row_max[:, :, None]), 0.0)
    denom = lax.optimization_barrier(jnp.sum(probs, axis=2))
    weights = widen(probs.astype(jnp.bfloat16))
    accum = jnp.einsum('hqk,khe->qhe', weights, value_heads)
    attn = (accum / denom.T[:, :, None]).reshape(SEQ, FEAT).astype(jnp.bfloat16)
    log_norm = row_max + jnp.log(denom)
    output = jnp.dot(attn, out_weight, preferred_element_type=jnp.float32)
    error = jnp.where(live[:, None], output - target_rows.astype(jnp.float32), 0.0)
    grad_out = (2.0 * error).astype(jnp.bfloat16)
    attn_wide = widen(attn)
    grad_wide = widen(grad_out)
    weight_part = jnp.einsum('tf,td->fd', attn_wide, grad_wide)
    grad_attn = jnp.einsum('td,fd->tf', grad_wide, out_weight.astype(jnp.float32)).astype(jnp.bfloat16)
    grad_attn_wide = widen(grad_attn)
    delta = lax.optimization_barrier(jnp.sum((grad_attn_wide * attn_wide).reshape(SEQ, HEADS, HEAD_DIM), axis=2)).T
    back_probs = jnp.where(allowed, jnp.exp(masked - log_norm[:, :, None]), 0.0)
    grad_heads = grad_attn_wide.reshape(SEQ, HEADS, HEAD_DIM)
    dprobs = jnp.einsum('qhe,khe->hqk', grad_heads, value_heads)
    dscores = widen((back_probs * (dprobs - delta[:, :, None])).astype(jnp.bfloat16))
    query_raw = jnp.einsum('hqk,khe->qhe', dscores, key_heads) * score_scale
    key_raw = jnp.einsum('hqk,qhe->khe', dscores, query_heads) * score_scale
    back_weights = widen(back_probs.astype(jnp.bfloat16))
    value_raw = jnp.einsum('hqk,qhe->khe', back_weights, grad_heads)
    return (query_raw.reshape(SEQ, FEAT), key_raw.reshape(SEQ, FEAT), value_raw.reshape(SEQ, FEAT), weight_part, jnp.sum(error * error))

def reference(query_rows, key_rows, value_rows, out_weight, target, lengths, segments):

    def per_sample(packed):
        return one_sample(packed, out_weight)
    results = lax.map(per_sample, (query_rows, key_rows, value_rows, target, lengths, segments))
    count = jnp.sum(lengths).astype(jnp.float32)
    ratio = jnp.float32(SAMPLES * SEQ) / count
    query_grad = ratio * results[0]
    key_grad = ratio * results[1]
    value_grad = ratio * results[2]
    weight_grad = lax.optimization_barrier(jnp.sum(results[3], axis=0)) * (ratio / SEQ)
    loss = jnp.sum(results[4]) / (count * WIDTH)
    return (query_grad, key_grad, value_grad, weight_grad, loss)
```

```python
import functools
import math

import jax
import jax.numpy as jnp
from jax import lax
from jax.experimental import pallas as pl
from jax.experimental.pallas import tpu as pltpu
from jax.sharding import Mesh
from jax.sharding import PartitionSpec as P

WIDTH = 1152
HEADS = 8
HEAD_DIM = 72
FEAT = 576
TOK = 128
HP = 80
FP = HEADS * HP
PATCH = ("patch_0", "patch_1")
DP = ("dp_0", "dp_1")
DP_PATCH = ("dp_0", "dp_1", "patch_0", "patch_1")
NEG_LARGE = -1e30
MESH = pl.DeviceIdType.MESH
BF = jnp.bfloat16
F32 = jnp.float32
ORDER = (4, 3, 5, 2, 6, 1, 7)
QTILE = 256
TILES = 4
KCH = 256
CHUNKS = 8


def mm(a, b):
    return jnp.dot(a, b, preferred_element_type=F32)


def mmt(a, b):
    return lax.dot_general(a, b, (((1,), (1,)), ((), ())), preferred_element_type=F32)


def eye(n):
    r = lax.broadcasted_iota(jnp.int32, (n, n), 0)
    c = lax.broadcasted_iota(jnp.int32, (n, n), 1)
    return jnp.where(r == c, 1.0, 0.0).astype(BF)


def lanes(i, n):
    return pl.ds(pl.multiple_of(i * n, n), n)


def kernel(
    q_ref, k_ref, v_ref, w_ref, tgt_ref, len_ref, seg_ref,
    dq_ref, dk_ref, dv_ref, attn_out, gt_out, loss_ref,
    e_ref, snd, rx, sib, segs, qt, kt, vt, km, vm, gk, gq, s_ref, p_ref, ds_ref, rden,
    w_pad, w_tr, tgt_tr, attn_snd, attn_rx, go_snd, go_rx, gos, q_snd, xs_snd, xs_rx, own,
    kv_snd, grad_rx,
    ssem, rsem,
):
    y = lax.axis_index("patch_0")
    c = lax.axis_index("patch_1")
    chip = lambda d: lax.rem(y + d, 8)
    at = lambda h: {"patch_0": h}
    sibling = {"patch_1": 1 - c}
    barrier = pltpu.get_barrier_semaphore()
    for d in range(1, 8):
        pl.semaphore_signal(barrier, inc=1, device_id=at(chip(d)), device_id_type=MESH)
    pl.semaphore_signal(barrier, inc=1, device_id=sibling, device_id_type=MESH)

    def send(kind, slot, src, dst, to, dslot):
        return pltpu.make_async_remote_copy(
            src_ref=src, dst_ref=dst, send_sem=ssem.at[kind, slot], recv_sem=rsem.at[kind, dslot],
            device_id=to, device_id_type=MESH)

    for h in range(HEADS):
        r = lax.broadcasted_iota(jnp.int32, (HP, FEAT), 0)
        f = lax.broadcasted_iota(jnp.int32, (HP, FEAT), 1)
        hit = jnp.logical_and(f - r == HEAD_DIM * h, r < HEAD_DIM)
        e_ref[h * HP:(h + 1) * HP, :] = jnp.where(hit, 1.0, 0.0).astype(BF)
    spread = e_ref[...]
    for j, ref in enumerate((q_ref, k_ref, v_ref)):
        snd[:, j * HP:(j + 1) * HP, :] = mmt(spread, ref[...]).astype(BF).reshape(HEADS, HP, TOK)
    segs[0, y] = seg_ref[...]
    rx[y] = snd[y]

    pl.semaphore_wait(barrier, 8)
    for d in ORDER:
        h = chip(d)
        send(0, h, snd.at[h], rx.at[y], at(h), y).start()
        send(1, h, seg_ref, segs.at[0, y], at(h), y).start()
    send(2, y, snd.at[y, HP:3 * HP], sib.at[y], sibling, y).start()
    send(3, y, seg_ref, segs.at[1, y], sibling, y).start()

    id256 = eye(256)
    id128 = eye(128)
    w_pad[...] = mm(spread, w_ref[...]).astype(BF)
    for j in range(5):
        n = 256 if j < 4 else 128
        cols = slice(256 * j, 256 * j + n)
        unit = id256 if n == 256 else id128
        w_tr[cols, :] = mmt(unit, w_pad[:, cols]).astype(BF)
        tgt_tr[cols, :] = mmt(unit, tgt_ref[:, cols]).astype(BF)
    length = len_ref[0]

    def place(block, number, parity, source, kv_t):
        kb, vb = kv_t[0:HP], kv_t[HP:2 * HP]
        kt[:, lanes(block, TOK)] = kb
        vt[:, lanes(block, TOK)] = vb
        rows = lanes(block, TOK)
        km[rows, :] = mmt(id128, kb).astype(BF)
        vm[rows, :] = mmt(id128, vb).astype(BF)
        at_pos = number * TOK + lax.broadcasted_iota(jnp.int32, (1, TOK), 1)
        group = jnp.where(at_pos < length, segs[parity, source], -1).astype(F32)
        spread_rows = jnp.broadcast_to(group, (TOK, TOK)).astype(BF)
        gk[rows, :] = mmt(id128, spread_rows)
        return group

    def place_own(source):
        block = rx[source]
        qt[:, lanes(source, TOK)] = block[0:HP]
        group = place(source, 2 * source + c, 0, source, block[HP:3 * HP])
        gq[:, lanes(source, TOK)] = group

    place_own(y)
    for d in ORDER:
        s = chip(d)
        send(0, s, snd.at[s], rx.at[s], at(s), s).wait_recv()
        send(1, s, seg_ref, segs.at[0, s], at(s), s).wait_recv()
        send(2, s, rx.at[s, HP:3 * HP], sib.at[s], sibling, s).start()
        send(3, s, segs.at[0, s], segs.at[1, s], sibling, s).start()
        place_own(s)
    for d in (0,) + ORDER:
        s = chip(d)
        send(2, s, rx.at[s, HP:3 * HP], sib.at[s], sibling, s).wait_recv()
        send(3, s, segs.at[0, s], segs.at[1, s], sibling, s).wait_recv()
        place(8 + s, 2 * s + 1 - c, 1, s, sib[s])

    scale = 1.0 / math.sqrt(HEAD_DIM)
    to_two = scale / math.log(2.0)

    def chunk(i):
        return pl.ds(pl.multiple_of(i * KCH, KCH), KCH)

    @pl.loop(0, TILES)
    def _(t):
        own_q = qt[:, lanes(t, QTILE)]
        own_g = gq[:, lanes(t, QTILE)]

        def first(i, top):
            sc = mm(km[chunk(i), :], own_q)
            g = gk[chunk(i), :]
            sc = jnp.where(jnp.concatenate([g, g], axis=1) == own_g, sc, NEG_LARGE)
            s_ref[chunk(i), :] = sc
            return jnp.maximum(top, jnp.max(sc, axis=0, keepdims=True))

        top = lax.fori_loop(0, CHUNKS, first, jnp.full((1, QTILE), NEG_LARGE, F32))

        def second(i, total):
            pr = jnp.exp2((s_ref[chunk(i), :] - top) * to_two)
            p_ref[t, chunk(i), :] = pr.astype(BF)
            return total + jnp.sum(pr, axis=0, keepdims=True)

        total = lax.fori_loop(0, CHUNKS, second, jnp.zeros((1, QTILE), F32))
        inv = 1.0 / total
        rden[t] = inv
        out = (mm(vt[...], p_ref[t]) * inv).astype(BF)
        for half in range(2):
            b = 2 * t + half
            attn_snd[b] = out[:, half * TOK:(half + 1) * TOK]

            @pl.when(b != y)
            def _():
                send(4, b, attn_snd.at[b], attn_rx.at[y], at(b), y).start()

    attn_rx[y] = attn_snd[y]
    for d in ORDER:
        s = chip(d)
        send(4, s, attn_snd.at[s], attn_rx.at[s], at(s), s).wait_recv()

    attn_t = attn_rx[...].reshape(FP, TOK)
    position = (2 * y + c) * TOK + lax.broadcasted_iota(jnp.int32, (1, TOK), 1)
    live = position < length
    out_t = mm(w_tr[...], attn_t)
    error = jnp.where(live, out_t - tgt_tr[...].astype(F32), 0.0)
    grad_t = (2.0 * error).astype(BF)
    gt_out[...] = grad_t
    go_snd[...] = mm(w_pad[...], grad_t).astype(BF).reshape(HEADS, HP, TOK)
    for d in ORDER:
        h = chip(d)
        send(5, h, go_snd.at[h], go_rx.at[y], at(h), y).start()
    go_rx[y] = go_snd[y]
    attn_out[...] = attn_t
    loss_ref[...] = jnp.sum(error * error, axis=0, keepdims=True)

    @pl.loop(0, TILES)
    def _(t):
        for half in range(2):
            b = 2 * t + half

            @pl.when(b != y)
            def _():
                send(5, b, go_snd.at[b], go_rx.at[b], at(b), b).wait_recv()

        both = jnp.concatenate([go_rx[2 * t], go_rx[2 * t + 1]], axis=1).astype(F32)
        scaled = (both * rden[t]).astype(BF)
        gos[t] = scaled
        attn = jnp.concatenate([attn_snd[2 * t], attn_snd[2 * t + 1]], axis=1)
        delta = jnp.sum(scaled.astype(F32) * attn.astype(F32), axis=0, keepdims=True)

        @pl.loop(0, CHUNKS)
        def _(i):
            dp = mm(vm[chunk(i), :], scaled)
            ds_ref[t, chunk(i), :] = (p_ref[t, chunk(i), :].astype(F32) * (dp - delta)).astype(BF)

        dq = (mm(kt[...], ds_ref[t]) * scale).astype(BF)
        for half in range(2):
            b = 2 * t + half
            q_snd[b] = dq[:, half * TOK:(half + 1) * TOK]

            @pl.when(b != y)
            def _():
                send(6, b, q_snd.at[b], grad_rx.at[y, 0:HP], at(b), y).start()

    def key_value(i):
        dk = jnp.zeros((HP, KCH), F32)
        dv = jnp.zeros((HP, KCH), F32)
        for t in range(TILES):
            dk = dk + mmt(qt[:, t * QTILE:(t + 1) * QTILE], ds_ref[t, chunk(i), :])
            dv = dv + mmt(gos[t], p_ref[t, chunk(i), :])
        return dk * scale, dv

    @pl.loop(0, 4)
    def _(i):
        dk, dv = key_value(i + 4)
        for half in range(2):
            b = 2 * i + half
            cols = slice(half * TOK, (half + 1) * TOK)
            xs_snd[b, 0:HP] = dk[:, cols].astype(BF)
            xs_snd[b, HP:2 * HP] = dv[:, cols].astype(BF)
            send(7, b, xs_snd.at[b], xs_rx.at[b], sibling, b).start()

    @pl.loop(0, 4)
    def _(i):
        dk, dv = key_value(i)
        for half in range(2):
            b = 2 * i + half
            cols = slice(half * TOK, (half + 1) * TOK)
            send(7, b, xs_snd.at[b], xs_rx.at[b], sibling, b).wait_recv()
            kv_snd[b, 0:HP] = (dk[:, cols] + xs_rx[b, 0:HP].astype(F32)).astype(BF)
            kv_snd[b, HP:2 * HP] = (dv[:, cols] + xs_rx[b, HP:2 * HP].astype(F32)).astype(BF)

            @pl.when(b != y)
            def _():
                send(8, b, kv_snd.at[b], grad_rx.at[y, HP:3 * HP], at(b), y).start()

    grad_rx[y, 0:HP] = q_snd[y]
    grad_rx[y, HP:3 * HP] = kv_snd[y]
    compact = jnp.zeros((FEAT, FP), BF)
    rows = []
    for h in range(HEADS):
        f = lax.broadcasted_iota(jnp.int32, (HEAD_DIM, FP), 0)
        r = lax.broadcasted_iota(jnp.int32, (HEAD_DIM, FP), 1)
        rows.append(jnp.where(r - f == HP * h, 1.0, 0.0))
    compact = jnp.concatenate(rows, axis=0).astype(BF)
    for d in ORDER:
        s = chip(d)
        send(6, s, q_snd.at[s], grad_rx.at[s, 0:HP], at(s), s).wait_recv()
        send(8, s, kv_snd.at[s], grad_rx.at[s, HP:3 * HP], at(s), s).wait_recv()
    for j, ref in enumerate((dq_ref, dk_ref, dv_ref)):
        got = grad_rx[:, j * HP:(j + 1) * HP, :].reshape(FP, TOK)
        ref[...] = mmt(id128, mm(compact, got).astype(BF))

    for d in (0,) + ORDER:
        s = chip(d)
        if d:
            send(0, s, snd.at[s], rx.at[y], at(s), y).wait_send()
            send(1, s, seg_ref, segs.at[0, y], at(s), y).wait_send()
            send(4, s, attn_snd.at[s], attn_rx.at[y], at(s), y).wait_send()
            send(5, s, go_snd.at[s], go_rx.at[y], at(s), y).wait_send()
            send(6, s, q_snd.at[s], grad_rx.at[y, 0:HP], at(s), y).wait_send()
            send(8, s, kv_snd.at[s], grad_rx.at[y, HP:3 * HP], at(s), y).wait_send()
        send(2, s, rx.at[s, HP:3 * HP], sib.at[s], sibling, s).wait_send()
        send(3, s, segs.at[0, s], segs.at[1, s], sibling, s).wait_send()
        send(7, s, xs_snd.at[s], xs_rx.at[s], sibling, s).wait_send()


def attention(q, k, v, w, target, lengths, segments):
    vm = pltpu.VMEM
    vmem = pl.BlockSpec(memory_space=pltpu.VMEM)
    keys = 16 * TOK
    return pl.pallas_call(
        kernel,
        out_shape=[
            jax.ShapeDtypeStruct((TOK, FEAT), F32),
            jax.ShapeDtypeStruct((TOK, FEAT), F32),
            jax.ShapeDtypeStruct((TOK, FEAT), F32),
            jax.ShapeDtypeStruct((FP, TOK), BF),
            jax.ShapeDtypeStruct((WIDTH, TOK), BF),
            jax.ShapeDtypeStruct((1, TOK), F32),
        ],
        in_specs=[vmem] * 5 + [pl.BlockSpec(memory_space=pltpu.SMEM), vmem],
        out_specs=[vmem] * 6,
        scratch_shapes=[
            vm((FP, FEAT), BF),
            vm((HEADS, 3 * HP, TOK), BF),
            vm((HEADS, 3 * HP, TOK), BF),
            vm((HEADS, 2 * HP, TOK), BF),
            vm((2, HEADS, 1, TOK), jnp.int32),
            vm((HP, 8 * TOK), BF),
            vm((HP, keys), BF),
            vm((HP, keys), BF),
            vm((keys, HP), BF),
            vm((keys, HP), BF),
            vm((keys, TOK), F32),
            vm((1, 8 * TOK), F32),
            vm((keys, QTILE), F32),
            vm((TILES, keys, QTILE), BF),
            vm((TILES, keys, QTILE), BF),
            vm((TILES, 1, QTILE), F32),
            vm((FP, WIDTH), BF),
            vm((WIDTH, FP), BF),
            vm((WIDTH, TOK), BF),
            vm((HEADS, HP, TOK), BF),
            vm((HEADS, HP, TOK), BF),
            vm((HEADS, HP, TOK), BF),
            vm((HEADS, HP, TOK), BF),
            vm((TILES, HP, QTILE), BF),
            vm((HEADS, HP, TOK), BF),
            vm((HEADS, 2 * HP, TOK), BF),
            vm((HEADS, 2 * HP, TOK), BF),
            vm((HEADS, 2 * HP, TOK), F32),
            vm((HEADS, 2 * HP, TOK), BF),
            vm((HEADS, 3 * HP, TOK), BF),
            pltpu.SemaphoreType.DMA((9, HEADS)),
            pltpu.SemaphoreType.DMA((9, HEADS)),
        ],
        compiler_params=pltpu.CompilerParams(
            collective_id=0, has_side_effects=True, vmem_limit_bytes=48 * 1024 * 1024),
        name="attention",
    )(q, k, v, w, target, lengths, segments)


def from_everyone(value, axis):
    copies = jnp.broadcast_to(value, (lax.axis_size(axis), *value.shape))
    return lax.all_to_all(copies, axis, split_axis=0, concat_axis=0, tiled=True)


def of_everyone(value, axis):
    return from_everyone(value, axis).sum(axis=0)


def in_blocks(value, dim, peers):
    shape = value.shape
    pieces = value.reshape(*shape[:dim], peers, shape[dim] // peers, *shape[dim + 1:])
    return jnp.moveaxis(pieces, dim, 0)


def sum_at_owner(value, axis, dim):
    peers = lax.axis_size(axis)
    pieces = lax.all_to_all(in_blocks(value, dim, peers), axis, 0, 0, tiled=True)
    return jnp.sum(pieces.astype(F32), axis=0)


def local(query_rows, key_rows, value_rows, out_weight, target, lengths, segments):
    groups = lax.axis_size(DP)
    total_rows = TOK * lax.axis_size(PATCH)
    dq, dk, dv, attn_t, grad_t, loss_part = attention(
        query_rows[0], key_rows[0], value_rows[0], out_weight, target[0], lengths, segments)
    weight_part = lax.dot_general(
        attn_t.reshape(HEADS, HP, TOK)[:, :HEAD_DIM].reshape(FEAT, TOK), grad_t,
        (((1,), (1,)), ((), ())), preferred_element_type=F32)
    stats = jnp.stack([jnp.sum(loss_part), lengths[0].astype(F32)])
    stats = of_everyone(of_everyone(stats, PATCH), DP)
    count = stats[1] / lax.axis_size(PATCH)
    row_share = sum_at_owner(weight_part.astype(BF), PATCH, 0)
    weight_share = sum_at_owner(row_share.astype(BF), DP, 1)
    ratio = jnp.float32(groups * total_rows) / count
    return (
        (ratio * dq)[None], (ratio * dk)[None], (ratio * dv)[None],
        weight_share * (ratio / total_rows), stats[0] / (count * WIDTH))


def solution(mesh):
    torus = Mesh(mesh.devices.reshape(4, 8, 8, 2), ("dp_0", "dp_1", "patch_0", "patch_1"))
    return jax.shard_map(
        local,
        mesh=torus,
        in_specs=(P(DP, PATCH, None), P(DP, PATCH, None), P(DP, PATCH, None), P(),
                  P(DP, PATCH, None), P(DP), P(DP, PATCH)),
        out_specs=(P(DP, PATCH, None), P(DP, PATCH, None), P(DP, PATCH, None), P(PATCH, DP), P()),
        check_vma=False,
    )
```

```python
import math

import jax
import jax.numpy as jnp
from jax import lax
from jax.experimental import pallas as pl
from jax.experimental.pallas import tpu as pltpu
from jax.sharding import Mesh
from jax.sharding import PartitionSpec as P

WIDTH = 1152
HEADS = 8
HEAD_DIM = 72
FEAT = 576
TOK = 128
HALF = 36
HALF_PAD = 48
LANES = HEADS * HALF_PAD
PATCH = ("patch_0", "patch_1")
DP = ("dp_0", "dp_1")
DP_PATCH = ("dp_0", "dp_1", "patch_0", "patch_1")
NEG_LARGE = -1e30
MESH = pl.DeviceIdType.MESH
BF = jnp.bfloat16
F32 = jnp.float32
ORDER = (4, 3, 5, 2, 6, 1, 7)
QTILE = 256
TILES = 4
KCH = 256
CHUNKS = 8


def mm(a, b):
    return jnp.dot(a, b, preferred_element_type=F32)


def mmt(a, b):
    return lax.dot_general(a, b, (((1,), (1,)), ((), ())), preferred_element_type=F32)


def eye(n):
    r = lax.broadcasted_iota(jnp.int32, (n, n), 0)
    c = lax.broadcasted_iota(jnp.int32, (n, n), 1)
    return jnp.where(r == c, 1.0, 0.0).astype(BF)


def lanes(i, n):
    return pl.ds(pl.multiple_of(i * n, n), n)


def up(n, m):
    return (n + m - 1) // m * m


def kernel(
    q_hbm, k_hbm, v_hbm, w_hbm, tgt_hbm, len_ref, seg_hbm,
    dq_ref, dk_ref, dv_ref, wg_ref, stat_ref,
    snd, w_ref, tgt_ref, rx, sib, segs, qt, kt, vt, km, vm, gk, gq, s_ref, p_ref, ds_ref, rden,
    w_tr, tgt_tr, attn_snd, attn_rx, go_snd, go_rx, gos, q_snd, xs_snd, xs_rx, kv_snd, grad_rx,
    gt, gt_sib, attn_sib, stats, x_snd, x_rx, x_sum, z_snd, z_rx, y_snd, y_rx,
    lsem, ssem, rsem,
):
    x = lax.axis_index("dp_0")
    z = lax.axis_index("dp_1")
    y = lax.axis_index("patch_0")
    c = lax.axis_index("patch_1")
    nx = lax.axis_size("dp_0")
    nz = lax.axis_size("dp_1")
    HD = HEAD_DIM
    chip = lambda d: lax.rem(y + d, 8)
    at = lambda h: {"patch_0": h}
    xs = [(lax.rem(x + d, nx)) for d in range(1, nx)]
    zs = [(lax.rem(z + d, nz)) for d in range(1, nz)]
    sibling = {"patch_1": 1 - c}
    barrier = pltpu.get_barrier_semaphore()
    for d in range(1, 8):
        pl.semaphore_signal(barrier, inc=1, device_id=at(chip(d)), device_id_type=MESH)
    pl.semaphore_signal(barrier, inc=1, device_id=sibling, device_id_type=MESH)
    for o in xs:
        pl.semaphore_signal(barrier, inc=1, device_id={"dp_0": o}, device_id_type=MESH)
    for o in zs:
        pl.semaphore_signal(barrier, inc=1, device_id={"dp_1": o}, device_id_type=MESH)

    loads = [
        pltpu.make_async_copy(src, dst, lsem.at[i])
        for i, (src, dst) in enumerate((
            (q_hbm, snd.at[0]), (k_hbm, snd.at[1]), (v_hbm, snd.at[2]), (seg_hbm, segs.at[0, y]),
            (w_hbm, w_ref), (tgt_hbm, tgt_ref)))
    ]
    for load in loads:
        load.start()

    def send(kind, slot, src, dst, to, dslot):
        return pltpu.make_async_remote_copy(
            src_ref=src, dst_ref=dst, send_sem=ssem.at[kind, slot], recv_sem=rsem.at[kind, dslot],
            device_id=to, device_id_type=MESH)

    for load in loads[:4]:
        load.wait()
    pl.semaphore_wait(barrier, 8 + len(xs) + len(zs))
    own_rows = [snd.at[:, y]]
    for d in ORDER:
        h = chip(d)
        send(0, h, snd.at[:, h], rx.at[y], at(h), y).start()
        send(1, h, segs.at[0, y], segs.at[0, y], at(h), y).start()
    send(2, y, snd.at[1:3, y], sib.at[y], sibling, y).start()
    send(3, y, segs.at[0, y], segs.at[1, y], sibling, y).start()

    id256 = eye(256)
    id128 = eye(128)
    loads[4].wait()
    loads[5].wait()
    for j in range(5):
        n = 256 if j < 4 else 128
        cols = slice(256 * j, 256 * j + n)
        unit = id256 if n == 256 else id128
        w_tr[cols, :] = mmt(unit, w_ref[:, cols]).astype(BF)
        tgt_tr[cols, :] = mmt(unit, tgt_ref[:, cols]).astype(BF)
    length = len_ref[0]

    def place(block, number, parity, source, kb, vb):
        kt[:, lanes(block, TOK)] = kb
        vt[:, lanes(block, TOK)] = vb
        rows = lanes(block, TOK)
        km[rows, :] = mmt(id128, kb).astype(BF)
        vm[rows, :] = mmt(id128, vb).astype(BF)
        at_pos = number * TOK + lax.broadcasted_iota(jnp.int32, (1, TOK), 1)
        group = jnp.where(at_pos < length, segs[parity, source], -1).astype(F32)
        spread_rows = jnp.broadcast_to(group, (TOK, TOK)).astype(BF)
        gk[rows, :] = mmt(id128, spread_rows)
        return group

    def place_own(source, qb, kb, vb):
        qt[:, lanes(source, TOK)] = qb
        gq[:, lanes(source, TOK)] = place(source, 2 * source + c, 0, source, kb, vb)

    place_own(y, snd[0, y], snd[1, y], snd[2, y])
    for d in ORDER:
        s = chip(d)
        send(0, s, snd.at[:, s], rx.at[s], at(s), s).wait_recv()
        send(1, s, segs.at[0, y], segs.at[0, s], at(s), s).wait_recv()
        send(2, s, rx.at[s, 1:3], sib.at[s], sibling, s).start()
        send(3, s, segs.at[0, s], segs.at[1, s], sibling, s).start()
        place_own(s, rx[s, 0], rx[s, 1], rx[s, 2])
    for d in (0,) + ORDER:
        s = chip(d)
        send(2, s, rx.at[s, 1:3], sib.at[s], sibling, s).wait_recv()
        send(3, s, segs.at[0, s], segs.at[1, s], sibling, s).wait_recv()
        place(8 + s, 2 * s + 1 - c, 1, s, sib[s, 0], sib[s, 1])

    scale = 1.0 / math.sqrt(HEAD_DIM)
    to_two = scale / math.log(2.0)

    def chunk(i):
        return pl.ds(pl.multiple_of(i * KCH, KCH), KCH)

    @pl.loop(0, TILES)
    def _(t):
        own_q = qt[:, lanes(t, QTILE)]
        own_g = gq[:, lanes(t, QTILE)]

        def first(i, top):
            sc = mm(km[chunk(i), :], own_q)
            g = gk[chunk(i), :]
            sc = jnp.where(jnp.concatenate([g, g], axis=1) == own_g, sc, NEG_LARGE)
            s_ref[chunk(i), :] = sc
            return jnp.maximum(top, jnp.max(sc, axis=0, keepdims=True))

        top = lax.fori_loop(0, CHUNKS, first, jnp.full((1, QTILE), NEG_LARGE, F32))

        def second(i, total):
            pr = jnp.exp2((s_ref[chunk(i), :] - top) * to_two)
            p_ref[t, chunk(i), :] = pr.astype(BF)
            return total + jnp.sum(pr, axis=0, keepdims=True)

        total = lax.fori_loop(0, CHUNKS, second, jnp.zeros((1, QTILE), F32))
        inv = 1.0 / total
        rden[t] = inv
        out = (mm(vt[...], p_ref[t]) * inv).astype(BF)
        for half in range(2):
            b = 2 * t + half
            attn_snd[b] = out[:, half * TOK:(half + 1) * TOK]

            @pl.when(b != y)
            def _():
                send(4, b, attn_snd.at[b], attn_rx.at[y], at(b), y).start()

    attn_rx[y] = attn_snd[y]
    for d in ORDER:
        s = chip(d)
        send(4, s, attn_snd.at[s], attn_rx.at[s], at(s), s).wait_recv()

    attn_t = attn_rx[...].reshape(FEAT, TOK)
    position = (2 * y + c) * TOK + lax.broadcasted_iota(jnp.int32, (1, TOK), 1)
    live = position < length
    out_t = mm(w_tr[...], attn_t)
    error = jnp.where(live, out_t - tgt_tr[...].astype(F32), 0.0)
    grad_t = (2.0 * error).astype(BF)
    gt[...] = grad_t
    go_snd[...] = mm(w_ref[...], grad_t).astype(BF).reshape(HEADS, HD, TOK)
    for d in ORDER:
        h = chip(d)
        send(5, h, go_snd.at[h], go_rx.at[y], at(h), y).start()
    send(9, 0, gt, gt_sib, sibling, 0).start()
    send(10, 0, attn_rx, attn_sib, sibling, 0).start()
    go_rx[y] = go_snd[y]

    squares = jnp.sum(error * error, axis=0, keepdims=True)
    lens = jnp.full((1, TOK), length.astype(F32), F32)
    row = lax.broadcasted_iota(jnp.int32, (8, TOK), 0)
    stats[0, 0] = jnp.where(row == 0, squares, jnp.where(row == 1, lens, 0.0))
    send(11, 0, stats.at[0, 0], stats.at[0, 1], sibling, 0).start()
    parts = []
    for h in range(HEADS):
        r = lax.broadcasted_iota(jnp.int32, (HALF_PAD, FEAT), 0)
        f = lax.broadcasted_iota(jnp.int32, (HALF_PAD, FEAT), 1)
        hit = jnp.logical_and(f - r == HD * h + HALF * c, r < HALF)
        parts.append(jnp.where(hit, 1.0, 0.0).astype(BF))
    pick = jnp.concatenate(parts, axis=0)
    send(10, 0, attn_rx, attn_sib, sibling, 0).wait_recv()
    attn_both = jnp.concatenate(
        [mm(pick, attn_t), mm(pick, attn_sib[...].reshape(FEAT, TOK))], axis=1).astype(BF)
    send(9, 0, gt, gt_sib, sibling, 0).wait_recv()
    send(11, 0, stats.at[0, 0], stats.at[0, 1], sibling, 0).wait_recv()
    stats[1, x] = stats[0, 0] + stats[0, 1]
    cx = WIDTH // nx
    cz = cx // nz
    czp = up(cz, 16)
    for o in xs + [x]:
        rows = pl.ds(pl.multiple_of(o * cx, 32), cx)
        both = jnp.concatenate([gt[rows, :], gt_sib[rows, :]], axis=1)
        x_snd[o] = mmt(both, attn_both).astype(BF)
        if o is not x:
            send(12, o, x_snd.at[o], x_rx.at[x], {"dp_0": o}, x).start()
            send(13, o, stats.at[1, x], stats.at[1, x], {"dp_0": o}, x).start()

    @pl.loop(0, TILES)
    def _(t):
        for half in range(2):
            b = 2 * t + half

            @pl.when(b != y)
            def _():
                send(5, b, go_snd.at[b], go_rx.at[b], at(b), b).wait_recv()

        both = jnp.concatenate([go_rx[2 * t], go_rx[2 * t + 1]], axis=1).astype(F32)
        scaled = (both * rden[t]).astype(BF)
        gos[t] = scaled
        attn = jnp.concatenate([attn_snd[2 * t], attn_snd[2 * t + 1]], axis=1)
        delta = jnp.sum(scaled.astype(F32) * attn.astype(F32), axis=0, keepdims=True)

        @pl.loop(0, CHUNKS)
        def _(i):
            dp = mm(vm[chunk(i), :], scaled)
            ds_ref[t, chunk(i), :] = (p_ref[t, chunk(i), :].astype(F32) * (dp - delta)).astype(BF)

        dq = (mm(kt[...], ds_ref[t]) * scale).astype(BF)
        for half in range(2):
            b = 2 * t + half
            q_snd[b] = dq[:, half * TOK:(half + 1) * TOK]

            @pl.when(b != y)
            def _():
                send(6, b, q_snd.at[b], grad_rx.at[0, y], at(b), y).start()

    def key_value(i):
        dk = jnp.zeros((HD, KCH), F32)
        dv = jnp.zeros((HD, KCH), F32)
        for t in range(TILES):
            dk = dk + mmt(qt[:, t * QTILE:(t + 1) * QTILE], ds_ref[t, chunk(i), :])
            dv = dv + mmt(gos[t], p_ref[t, chunk(i), :])
        return dk * scale, dv

    @pl.loop(0, 4)
    def _(i):
        dk, dv = key_value(i + 4)
        for half in range(2):
            b = 2 * i + half
            cols = slice(half * TOK, (half + 1) * TOK)
            xs_snd[b, 0] = dk[:, cols].astype(BF)
            xs_snd[b, 1] = dv[:, cols].astype(BF)
            send(7, b, xs_snd.at[b], xs_rx.at[b], sibling, b).start()

    @pl.loop(0, 4)
    def _(i):
        dk, dv = key_value(i)
        for half in range(2):
            b = 2 * i + half
            cols = slice(half * TOK, (half + 1) * TOK)
            send(7, b, xs_snd.at[b], xs_rx.at[b], sibling, b).wait_recv()
            kv_snd[b, 0] = (dk[:, cols] + xs_rx[b, 0].astype(F32)).astype(BF)
            kv_snd[b, 1] = (dv[:, cols] + xs_rx[b, 1].astype(F32)).astype(BF)

            @pl.when(b != y)
            def _():
                send(8, b, kv_snd.at[b], grad_rx.at[1:3, y], at(b), y).start()

    grad_rx[0, y] = q_snd[y]
    grad_rx[1, y] = kv_snd[y, 0]
    grad_rx[2, y] = kv_snd[y, 1]

    for o in xs:
        send(12, o, x_snd.at[o], x_rx.at[o], {"dp_0": o}, o).wait_recv()
        send(13, o, stats.at[1, x], stats.at[1, o], {"dp_0": o}, o).wait_recv()
    acc = x_snd[x].astype(F32)
    tot = stats[1, x]
    for o in xs:
        acc = acc + x_rx[o].astype(F32)
        tot = tot + stats[1, o]
    x_sum[...] = acc
    stats[2, z] = tot
    for k in range(nz):
        z_snd[k, 0:cz] = x_sum[k * cz:(k + 1) * cz, :].astype(BF)
        if czp > cz:
            z_snd[k, cz:czp] = jnp.zeros((czp - cz, LANES), BF)
    for o in zs:
        send(14, o, z_snd.at[o], z_rx.at[z], {"dp_1": o}, z).start()
        send(15, o, stats.at[2, z], stats.at[2, z], {"dp_1": o}, z).start()

    for d in ORDER:
        s = chip(d)
        send(6, s, q_snd.at[s], grad_rx.at[0, s], at(s), s).wait_recv()
    for o in zs:
        send(14, o, z_snd.at[o], z_rx.at[o], {"dp_1": o}, o).wait_recv()
        send(15, o, stats.at[2, z], stats.at[2, o], {"dp_1": o}, o).wait_recv()
    acc = z_snd[z].astype(F32)
    tot = stats[2, z]
    for o in zs:
        acc = acc + z_rx[o].astype(F32)
        tot = tot + stats[2, o]
    stats[3, y] = tot
    turned = mmt(eye(LANES), acc.astype(BF)).astype(BF)
    y_snd[:, :, 0:czp] = turned.reshape(HEADS, HALF_PAD, czp)
    for d in ORDER:
        h = chip(d)
        send(16, h, y_snd.at[h], y_rx.at[y], at(h), y).start()
        send(17, h, stats.at[3, y], stats.at[3, y], at(h), y).start()
    y_rx[y] = y_snd[y]
    for d in ORDER:
        s = chip(d)
        send(8, s, kv_snd.at[s], grad_rx.at[1:3, s], at(s), s).wait_recv()
        send(16, s, y_snd.at[s], y_rx.at[s], at(s), s).wait_recv()
        send(17, s, stats.at[3, y], stats.at[3, s], at(s), s).wait_recv()
    tot = jnp.zeros((8, TOK), F32)
    acc = jnp.zeros((HALF_PAD, czp), F32)
    for s in range(8):
        tot = tot + stats[3, s]
        acc = acc + y_rx[s, :, 0:czp].astype(F32)
    stat_ref[...] = tot
    wg_ref[...] = acc[0:HALF, 0:cz]
    ratio = jnp.float32(16 * TOK * 16 * nx * nz) / tot[1:2]
    for j, ref in enumerate((dq_ref, dk_ref, dv_ref)):
        ref[...] = grad_rx[j].reshape(FEAT, TOK).astype(F32) * ratio

    for d in (0,) + ORDER:
        s = chip(d)
        if d:
            send(0, s, snd.at[:, s], rx.at[y], at(s), y).wait_send()
            send(1, s, segs.at[0, y], segs.at[0, y], at(s), y).wait_send()
            send(4, s, attn_snd.at[s], attn_rx.at[y], at(s), y).wait_send()
            send(5, s, go_snd.at[s], go_rx.at[y], at(s), y).wait_send()
            send(6, s, q_snd.at[s], grad_rx.at[0, y], at(s), y).wait_send()
            send(8, s, kv_snd.at[s], grad_rx.at[1:3, y], at(s), y).wait_send()
            send(16, s, y_snd.at[s], y_rx.at[y], at(s), y).wait_send()
            send(17, s, stats.at[3, y], stats.at[3, y], at(s), y).wait_send()
        send(2, s, rx.at[s, 1:3], sib.at[s], sibling, s).wait_send()
        send(3, s, segs.at[0, s], segs.at[1, s], sibling, s).wait_send()
        send(7, s, xs_snd.at[s], xs_rx.at[s], sibling, s).wait_send()
    send(9, 0, gt, gt_sib, sibling, 0).wait_send()
    send(10, 0, attn_rx, attn_sib, sibling, 0).wait_send()
    send(11, 0, stats.at[0, 0], stats.at[0, 1], sibling, 0).wait_send()
    for o in xs:
        send(12, o, x_snd.at[o], x_rx.at[x], {"dp_0": o}, x).wait_send()
        send(13, o, stats.at[1, x], stats.at[1, x], {"dp_0": o}, x).wait_send()
    for o in zs:
        send(14, o, z_snd.at[o], z_rx.at[z], {"dp_1": o}, z).wait_send()
        send(15, o, stats.at[2, z], stats.at[2, z], {"dp_1": o}, z).wait_send()


def attention(q, k, v, w, target, lengths, segments):
    vm = pltpu.VMEM
    vmem = pl.BlockSpec(memory_space=pltpu.VMEM)
    hbm = pl.BlockSpec(memory_space=pl.ANY)
    keys = 16 * TOK
    nx = lax.axis_size("dp_0")
    nz = lax.axis_size("dp_1")
    cx = WIDTH // nx
    cz = cx // nz
    czp = up(cz, 16)
    HD = HEAD_DIM
    heads_of = lambda n: vm((HEADS, HD, TOK) if n is None else (HEADS, n, HD, TOK), BF)
    return pl.pallas_call(
        kernel,
        out_shape=[jax.ShapeDtypeStruct((FEAT, TOK), F32)] * 3 + [
            jax.ShapeDtypeStruct((HALF, cz), F32),
            jax.ShapeDtypeStruct((8, TOK), F32),
        ],
        in_specs=[hbm] * 5 + [pl.BlockSpec(memory_space=pltpu.SMEM), hbm],
        out_specs=[vmem] * 5,
        scratch_shapes=[
            vm((3, HEADS, HD, TOK), BF),
            vm((FEAT, WIDTH), BF),
            vm((TOK, WIDTH), BF),
            heads_of(3),
            heads_of(2),
            vm((2, HEADS, 1, TOK), jnp.int32),
            vm((HD, 8 * TOK), BF),
            vm((HD, keys), BF),
            vm((HD, keys), BF),
            vm((keys, HD), BF),
            vm((keys, HD), BF),
            vm((keys, TOK), F32),
            vm((1, 8 * TOK), F32),
            vm((keys, QTILE), F32),
            vm((TILES, keys, QTILE), BF),
            vm((TILES, keys, QTILE), BF),
            vm((TILES, 1, QTILE), F32),
            vm((WIDTH, FEAT), BF),
            vm((WIDTH, TOK), BF),
            heads_of(None),
            heads_of(None),
            heads_of(None),
            heads_of(None),
            vm((TILES, HD, QTILE), BF),
            heads_of(None),
            heads_of(2),
            heads_of(2),
            heads_of(2),
            vm((3, HEADS, HD, TOK), BF),
            vm((WIDTH, TOK), BF),
            vm((WIDTH, TOK), BF),
            heads_of(None),
            vm((4, 8, 8, TOK), F32),
            vm((nx, cx, LANES), BF),
            vm((nx, cx, LANES), BF),
            vm((cx, LANES), F32),
            vm((nz, czp, LANES), BF),
            vm((nz, czp, LANES), BF),
            vm((HEADS, HALF_PAD, up(czp, 128)), BF),
            vm((HEADS, HALF_PAD, up(czp, 128)), BF),
            pltpu.SemaphoreType.DMA((6,)),
            pltpu.SemaphoreType.DMA((18, 8)),
            pltpu.SemaphoreType.DMA((18, 8)),
        ],
        compiler_params=pltpu.CompilerParams(
            collective_id=0, has_side_effects=True, vmem_limit_bytes=62 * 1024 * 1024),
        name="attention",
    )(q, k, v, w, target, lengths, segments)


def local(query_rows, key_rows, value_rows, out_weight, target, lengths, segments):
    groups = lax.axis_size(DP)
    total_rows = TOK * lax.axis_size(PATCH)
    by_head = lambda rows: rows[0].T.reshape(HEADS, HEAD_DIM, TOK)
    dq, dk, dv, weight, stats = attention(
        by_head(query_rows), by_head(key_rows), by_head(value_rows), out_weight, target[0],
        lengths, segments)
    count = stats[1, 0] / lax.axis_size(PATCH)
    ratio = jnp.float32(groups * total_rows) / count
    loss = jnp.sum(stats[0]) / (count * WIDTH)
    return (dq.T[None], dk.T[None], dv.T[None], weight * (ratio / total_rows), loss)


def solution(mesh):
    torus = Mesh(mesh.devices.reshape(4, 8, 8, 2), ("dp_0", "dp_1", "patch_0", "patch_1"))
    return jax.shard_map(
        local,
        mesh=torus,
        in_specs=(P(DP, PATCH, None), P(DP, PATCH, None), P(DP, PATCH, None), P(),
                  P(DP, PATCH, None), P(DP), P(DP, PATCH)),
        out_specs=(P(DP, PATCH, None), P(DP, PATCH, None), P(DP, PATCH, None), P(PATCH, DP), P()),
        check_vma=False,
    )
```

```python
import math

import jax
import jax.numpy as jnp
from jax import lax
from jax.experimental import pallas as pl
from jax.experimental.pallas import tpu as pltpu
from jax.sharding import Mesh
from jax.sharding import PartitionSpec as P

WIDTH = 1152
HEADS = 8
HEAD_DIM = 72
FEAT = 576
TOK = 128
HALF = 36
HALF_PAD = 48
LANES = HEADS * HALF_PAD
PATCH = ("patch_0", "patch_1")
DP = ("dp_0", "dp_1")
DP_PATCH = ("dp_0", "dp_1", "patch_0", "patch_1")
NEG_LARGE = -1e30
MESH = pl.DeviceIdType.MESH
BF = jnp.bfloat16
F32 = jnp.float32
ORDER = (4, 3, 5, 2, 6, 1, 7)
QTILE = 256
TILES = 4
FAR_FIRST = (2, 1, 3, 0)
NEAR_FIRST = (0, 1, 3, 2)
KCH = 256
CHUNKS = 8


def mm(a, b):
    return jnp.dot(a, b, preferred_element_type=F32)


def mmt(a, b):
    return lax.dot_general(a, b, (((1,), (1,)), ((), ())), preferred_element_type=F32)


def eye(n):
    r = lax.broadcasted_iota(jnp.int32, (n, n), 0)
    c = lax.broadcasted_iota(jnp.int32, (n, n), 1)
    return jnp.where(r == c, 1.0, 0.0).astype(BF)


def lanes(i, n):
    return pl.ds(pl.multiple_of(i * n, n), n)


def up(n, m):
    return (n + m - 1) // m * m


def kernel(
    q_hbm, k_hbm, v_hbm, w_hbm, tgt_hbm, len_ref, seg_hbm,
    grad_rx, wg_ref, stat_ref,
    snd, w_ref, tgt_ref, rx, sib, segs, qt, kt, vt, km, vm, gk, gq, s_ref, p_ref, ds_ref, rden,
    w_tr, tgt_tr, attn_snd, attn_rx, go_snd, go_rx, gos, q_snd, xs_snd, xs_rx, kv_snd,
    gt, gt_sib, attn_sib, stats, x_snd, x_rx, x_sum, z_snd, z_rx, y_snd, y_rx,
    lsem, ssem, rsem,
):
    x = lax.axis_index("dp_0")
    z = lax.axis_index("dp_1")
    y = lax.axis_index("patch_0")
    c = lax.axis_index("patch_1")
    nx = lax.axis_size("dp_0")
    nz = lax.axis_size("dp_1")
    HD = HEAD_DIM
    chip = lambda d: lax.rem(y + d, 8)
    at = lambda h: {"patch_0": h}
    xs = [(lax.rem(x + d, nx)) for d in range(1, nx)]
    zs = [(lax.rem(z + d, nz)) for d in range(1, nz)]
    sibling = {"patch_1": 1 - c}
    barrier = pltpu.get_barrier_semaphore()
    for d in range(1, 8):
        pl.semaphore_signal(barrier, inc=1, device_id=at(chip(d)), device_id_type=MESH)
    pl.semaphore_signal(barrier, inc=1, device_id=sibling, device_id_type=MESH)
    for o in xs:
        pl.semaphore_signal(barrier, inc=1, device_id={"dp_0": o}, device_id_type=MESH)
    for o in zs:
        pl.semaphore_signal(barrier, inc=1, device_id={"dp_1": o}, device_id_type=MESH)

    loads = [
        pltpu.make_async_copy(src, dst, lsem.at[i])
        for i, (src, dst) in enumerate((
            (q_hbm, snd.at[0]), (k_hbm, snd.at[1]), (v_hbm, snd.at[2]), (seg_hbm, segs.at[0, y]),
            (w_hbm, w_ref), (tgt_hbm, tgt_ref)))
    ]
    for load in loads:
        load.start()

    def send(kind, slot, src, dst, to, dslot):
        return pltpu.make_async_remote_copy(
            src_ref=src, dst_ref=dst, send_sem=ssem.at[kind, slot], recv_sem=rsem.at[kind, dslot],
            device_id=to, device_id_type=MESH)

    for load in loads[:4]:
        load.wait()
    pl.semaphore_wait(barrier, 8 + len(xs) + len(zs))
    own_rows = [snd.at[:, y]]
    for d in ORDER:
        h = chip(d)
        send(0, h, snd.at[:, h], rx.at[y], at(h), y).start()
        send(1, h, segs.at[0, y], segs.at[0, y], at(h), y).start()
    send(2, y, snd.at[1:3, y], sib.at[y], sibling, y).start()
    send(3, y, segs.at[0, y], segs.at[1, y], sibling, y).start()

    id256 = eye(256)
    id128 = eye(128)
    loads[4].wait()
    loads[5].wait()
    for j in range(5):
        n = 256 if j < 4 else 128
        cols = slice(256 * j, 256 * j + n)
        unit = id256 if n == 256 else id128
        w_tr[cols, :] = mmt(unit, w_ref[:, cols]).astype(BF)
        tgt_tr[cols, :] = mmt(unit, tgt_ref[:, cols]).astype(BF)
    length = len_ref[0]

    def place(block, number, parity, source, kb, vb):
        kt[:, lanes(block, TOK)] = kb
        vt[:, lanes(block, TOK)] = vb
        rows = lanes(block, TOK)
        km[rows, :] = mmt(id128, kb).astype(BF)
        vm[rows, :] = mmt(id128, vb).astype(BF)
        at_pos = number * TOK + lax.broadcasted_iota(jnp.int32, (1, TOK), 1)
        group = jnp.where(at_pos < length, segs[parity, source], -1).astype(F32)
        spread_rows = jnp.broadcast_to(group, (TOK, TOK)).astype(BF)
        gk[rows, :] = mmt(id128, spread_rows)
        return group

    def place_own(source, qb, kb, vb):
        qt[:, lanes(source, TOK)] = qb
        gq[:, lanes(source, TOK)] = place(source, 2 * source + c, 0, source, kb, vb)

    def place_sibling(source):
        send(2, source, rx.at[source, 1:3], sib.at[source], sibling, source).wait_recv()
        send(3, source, segs.at[0, source], segs.at[1, source], sibling, source).wait_recv()
        place(8 + source, 2 * source + 1 - c, 1, source, sib[source, 0], sib[source, 1])

    place_own(y, snd[0, y], snd[1, y], snd[2, y])
    before = y
    for d in ORDER:
        s = chip(d)
        send(0, s, snd.at[:, s], rx.at[s], at(s), s).wait_recv()
        send(1, s, segs.at[0, y], segs.at[0, s], at(s), s).wait_recv()
        send(2, s, rx.at[s, 1:3], sib.at[s], sibling, s).start()
        send(3, s, segs.at[0, s], segs.at[1, s], sibling, s).start()
        place_own(s, rx[s, 0], rx[s, 1], rx[s, 2])
        place_sibling(before)
        before = s
    place_sibling(before)

    scale = 1.0 / math.sqrt(HEAD_DIM)
    to_two = scale / math.log(2.0)

    def chunk(i):
        return pl.ds(pl.multiple_of(i * KCH, KCH), KCH)

    pair = y // 2

    def nth(order, n):
        first = jnp.where(n == 0, order[0], jnp.where(n == 1, order[1], jnp.where(n == 2, order[2], order[3])))
        return lax.rem(pair + first, TILES)

    def fold(v, op):
        n = v.shape[0] // 8
        parts = [v[8 * i:8 * i + 8] for i in range(n)]
        while len(parts) > 1:
            parts = [op(*parts[i:i + 2]) if i + 1 < len(parts) else parts[i] for i in range(0, len(parts), 2)]
        return parts[0]

    @pl.loop(0, TILES)
    def _(n):
        t = nth(FAR_FIRST, n)
        own_q = qt[:, lanes(t, QTILE)]
        own_g = gq[:, lanes(t, QTILE)]
        top = jnp.full((8, QTILE), NEG_LARGE, F32)
        for i in range(CHUNKS):
            part = slice(i * KCH, (i + 1) * KCH)
            sc = mm(km[part, :], own_q)
            g = gk[part, :]
            sc = jnp.where(jnp.concatenate([g, g], axis=1) == own_g, sc, NEG_LARGE)
            s_ref[part, :] = sc
            top = jnp.maximum(top, fold(sc, jnp.maximum))
        top = jnp.max(top, axis=0, keepdims=True)
        total = jnp.zeros((8, QTILE), F32)
        for i in range(CHUNKS):
            part = slice(i * KCH, (i + 1) * KCH)
            pr = jnp.exp2((s_ref[part, :] - top) * to_two)
            p_ref[t, part, :] = pr.astype(BF)
            total = total + fold(pr, jnp.add)
        inv = 1.0 / jnp.sum(total, axis=0, keepdims=True)
        rden[t] = inv
        out = (mm(vt[...], p_ref[t]) * inv).astype(BF)
        for half in range(2):
            b = 2 * t + half
            attn_snd[b] = out[:, half * TOK:(half + 1) * TOK]

            @pl.when(b != y)
            def _():
                send(4, b, attn_snd.at[b], attn_rx.at[y], at(b), y).start()

    attn_rx[y] = attn_snd[y]
    for d in ORDER:
        s = chip(d)
        send(4, s, attn_snd.at[s], attn_rx.at[s], at(s), s).wait_recv()

    send(10, 0, attn_rx, attn_sib, sibling, 0).start()
    attn_t = attn_rx[...].reshape(FEAT, TOK)
    position = (2 * y + c) * TOK + lax.broadcasted_iota(jnp.int32, (1, TOK), 1)
    live = position < length
    out_t = mm(w_tr[...], attn_t)
    error = jnp.where(live, out_t - tgt_tr[...].astype(F32), 0.0)
    grad_t = (2.0 * error).astype(BF)
    gt[...] = grad_t
    squares = jnp.sum(fold(error * error, jnp.add), axis=0, keepdims=True)
    lens = jnp.full((1, TOK), length.astype(F32), F32)
    row = lax.broadcasted_iota(jnp.int32, (8, TOK), 0)
    stats[0, 0] = jnp.where(row == 0, squares, jnp.where(row == 1, lens, 0.0))
    send(9, 0, gt, gt_sib, sibling, 0).start()
    send(11, 0, stats.at[0, 0], stats.at[0, 1], sibling, 0).start()
    go_snd[...] = mm(w_ref[...], grad_t).astype(BF).reshape(HEADS, HD, TOK)
    for d in ORDER:
        h = chip(d)
        send(5, h, go_snd.at[h], go_rx.at[y], at(h), y).start()
    go_rx[y] = go_snd[y]

    parts = []
    for h in range(HEADS):
        r = lax.broadcasted_iota(jnp.int32, (HALF_PAD, FEAT), 0)
        f = lax.broadcasted_iota(jnp.int32, (HALF_PAD, FEAT), 1)
        hit = jnp.logical_and(f - r == HD * h + HALF * c, r < HALF)
        parts.append(jnp.where(hit, 1.0, 0.0).astype(BF))
    pick = jnp.concatenate(parts, axis=0)
    send(10, 0, attn_rx, attn_sib, sibling, 0).wait_recv()
    attn_both = jnp.concatenate(
        [mm(pick, attn_t), mm(pick, attn_sib[...].reshape(FEAT, TOK))], axis=1).astype(BF)
    send(9, 0, gt, gt_sib, sibling, 0).wait_recv()
    send(11, 0, stats.at[0, 0], stats.at[0, 1], sibling, 0).wait_recv()
    stats[1, x] = stats[0, 0] + stats[0, 1]
    cx = WIDTH // nx
    cz = cx // nz
    czp = up(cz, 8)
    ch = cx // 2
    for half in range(2):
        for o in xs + [x]:
            rows = pl.ds(pl.multiple_of(o * cx + half * ch, 16), ch)
            both = jnp.concatenate([gt[rows, :], gt_sib[rows, :]], axis=1)
            x_snd[half, o] = mmt(both, attn_both).astype(BF)
            if o is not x:
                send(12 + half, o, x_snd.at[half, o], x_rx.at[half, x], {"dp_0": o}, x).start()
                if half == 0:
                    send(18, o, stats.at[1, x], stats.at[1, x], {"dp_0": o}, x).start()

    def sum_over_x(half):
        for o in xs:
            send(12 + half, o, x_snd.at[half, o], x_rx.at[half, o], {"dp_0": o}, o).wait_recv()
        acc = x_snd[half, x].astype(F32)
        for o in xs:
            acc = acc + x_rx[half, o].astype(F32)
        x_sum[half] = acc
        for k in range(nz // 2):
            to = half * (nz // 2) + k
            z_snd[to, 0:cz] = x_sum[half, k * cz:(k + 1) * cz, :].astype(BF)
            if czp > cz:
                z_snd[to, cz:czp] = jnp.zeros((czp - cz, LANES), BF)

            @pl.when(to != z)
            def _():
                send(14, to, z_snd.at[to], z_rx.at[z], {"dp_1": to}, z).start()

    @pl.loop(0, TILES)
    def _(n):
        t = nth(NEAR_FIRST, n)
        for half in range(2):
            b = 2 * t + half

            @pl.when(b != y)
            def _():
                send(5, b, go_snd.at[b], go_rx.at[b], at(b), b).wait_recv()

        both = jnp.concatenate([go_rx[2 * t], go_rx[2 * t + 1]], axis=1).astype(F32)
        scaled = (both * rden[t]).astype(BF)
        gos[t] = scaled
        attn = jnp.concatenate([attn_snd[2 * t], attn_snd[2 * t + 1]], axis=1)
        delta = jnp.sum(scaled.astype(F32) * attn.astype(F32), axis=0, keepdims=True)
        for i in range(CHUNKS):
            part = slice(i * KCH, (i + 1) * KCH)
            dp = mm(vm[part, :], scaled)
            ds_ref[t, part, :] = (p_ref[t, part, :].astype(F32) * (dp - delta)).astype(BF)
        dq = (mm(kt[...], ds_ref[t]) * scale).astype(BF)
        for half in range(2):
            b = 2 * t + half
            q_snd[b] = dq[:, half * TOK:(half + 1) * TOK]

            @pl.when(b != y)
            def _():
                send(6, b, q_snd.at[b], grad_rx.at[0, y], at(b), y).start()

    def key_value(i):
        dk = jnp.zeros((HD, KCH), F32)
        dv = jnp.zeros((HD, KCH), F32)
        for t in range(TILES):
            dk = dk + mmt(qt[:, t * QTILE:(t + 1) * QTILE], ds_ref[t, chunk(i), :])
            dv = dv + mmt(gos[t], p_ref[t, chunk(i), :])
        return dk * scale, dv

    for n in range(4):
        i = nth(FAR_FIRST, n)
        dk, dv = key_value(i + 4)
        for half in range(2):
            b = 2 * i + half
            cols = slice(half * TOK, (half + 1) * TOK)
            xs_snd[b, 0] = dk[:, cols].astype(BF)
            xs_snd[b, 1] = dv[:, cols].astype(BF)
            send(7, b, xs_snd.at[b], xs_rx.at[b], sibling, b).start()

    sum_over_x(0)
    for n in range(4):
        i = nth(FAR_FIRST, n)
        dk, dv = key_value(i)
        for half in range(2):
            b = 2 * i + half
            cols = slice(half * TOK, (half + 1) * TOK)
            send(7, b, xs_snd.at[b], xs_rx.at[b], sibling, b).wait_recv()
            kv_snd[b, 0] = (dk[:, cols] + xs_rx[b, 0].astype(F32)).astype(BF)
            kv_snd[b, 1] = (dv[:, cols] + xs_rx[b, 1].astype(F32)).astype(BF)

            @pl.when(b != y)
            def _():
                send(8, b, kv_snd.at[b], grad_rx.at[1:3, y], at(b), y).start()

    grad_rx[0, y] = q_snd[y]
    grad_rx[1, y] = kv_snd[y, 0]
    grad_rx[2, y] = kv_snd[y, 1]

    sum_over_x(1)
    tot = stats[1, x]
    for o in xs:
        send(18, o, stats.at[1, x], stats.at[1, o], {"dp_0": o}, o).wait_recv()
        tot = tot + stats[1, o]
    stats[2, z] = tot
    for o in zs:
        send(15, o, stats.at[2, z], stats.at[2, z], {"dp_1": o}, z).start()

    for d in ORDER:
        s = chip(d)
        send(6, s, q_snd.at[s], grad_rx.at[0, s], at(s), s).wait_recv()
    for o in zs:
        send(14, o, z_snd.at[o], z_rx.at[o], {"dp_1": o}, o).wait_recv()
        send(15, o, stats.at[2, z], stats.at[2, o], {"dp_1": o}, o).wait_recv()
    acc = z_snd[z].astype(F32)
    tot = stats[2, z]
    for o in zs:
        acc = acc + z_rx[o].astype(F32)
        tot = tot + stats[2, o]
    stats[3, y] = tot
    turned = mmt(eye(LANES), acc.astype(BF)).astype(BF)
    y_snd[:, :, 0:czp] = turned.reshape(HEADS, HALF_PAD, czp)
    for d in ORDER:
        h = chip(d)
        send(16, h, y_snd.at[h], y_rx.at[y], at(h), y).start()
        send(17, h, stats.at[3, y], stats.at[3, y], at(h), y).start()
    y_rx[y] = y_snd[y]
    for d in ORDER:
        s = chip(d)
        send(8, s, kv_snd.at[s], grad_rx.at[1:3, s], at(s), s).wait_recv()
        send(16, s, y_snd.at[s], y_rx.at[s], at(s), s).wait_recv()
        send(17, s, stats.at[3, y], stats.at[3, s], at(s), s).wait_recv()
    tot = jnp.zeros((8, TOK), F32)
    acc = jnp.zeros((HALF_PAD, czp), F32)
    for s in range(8):
        tot = tot + stats[3, s]
        acc = acc + y_rx[s, :, 0:czp].astype(F32)
    stat_ref[...] = tot
    wg_ref[...] = acc[0:HALF, 0:cz]

    for d in (0,) + ORDER:
        s = chip(d)
        if d:
            send(0, s, snd.at[:, s], rx.at[y], at(s), y).wait_send()
            send(1, s, segs.at[0, y], segs.at[0, y], at(s), y).wait_send()
            send(4, s, attn_snd.at[s], attn_rx.at[y], at(s), y).wait_send()
            send(5, s, go_snd.at[s], go_rx.at[y], at(s), y).wait_send()
            send(6, s, q_snd.at[s], grad_rx.at[0, y], at(s), y).wait_send()
            send(8, s, kv_snd.at[s], grad_rx.at[1:3, y], at(s), y).wait_send()
            send(16, s, y_snd.at[s], y_rx.at[y], at(s), y).wait_send()
            send(17, s, stats.at[3, y], stats.at[3, y], at(s), y).wait_send()
        send(2, s, rx.at[s, 1:3], sib.at[s], sibling, s).wait_send()
        send(3, s, segs.at[0, s], segs.at[1, s], sibling, s).wait_send()
        send(7, s, xs_snd.at[s], xs_rx.at[s], sibling, s).wait_send()
    send(9, 0, gt, gt_sib, sibling, 0).wait_send()
    send(10, 0, attn_rx, attn_sib, sibling, 0).wait_send()
    send(11, 0, stats.at[0, 0], stats.at[0, 1], sibling, 0).wait_send()
    for o in xs:
        send(12, o, x_snd.at[0, o], x_rx.at[0, x], {"dp_0": o}, x).wait_send()
        send(13, o, x_snd.at[1, o], x_rx.at[1, x], {"dp_0": o}, x).wait_send()
        send(18, o, stats.at[1, x], stats.at[1, x], {"dp_0": o}, x).wait_send()
    for o in zs:
        send(14, o, z_snd.at[o], z_rx.at[z], {"dp_1": o}, z).wait_send()
        send(15, o, stats.at[2, z], stats.at[2, z], {"dp_1": o}, z).wait_send()


def attention(q, k, v, w, target, lengths, segments):
    vm = pltpu.VMEM
    vmem = pl.BlockSpec(memory_space=pltpu.VMEM)
    hbm = pl.BlockSpec(memory_space=pltpu.HBM)
    keys = 16 * TOK
    nx = lax.axis_size("dp_0")
    nz = lax.axis_size("dp_1")
    cx = WIDTH // nx
    cz = cx // nz
    czp = up(cz, 8)
    HD = HEAD_DIM
    heads_of = lambda n: vm((HEADS, HD, TOK) if n is None else (HEADS, n, HD, TOK), BF)
    return pl.pallas_call(
        kernel,
        out_shape=[
            jax.ShapeDtypeStruct((3, HEADS, HD, TOK), BF),
            jax.ShapeDtypeStruct((HALF, cz), F32),
            jax.ShapeDtypeStruct((8, TOK), F32),
        ],
        in_specs=[hbm] * 5 + [pl.BlockSpec(memory_space=pltpu.SMEM), hbm],
        out_specs=[vmem] * 3,
        scratch_shapes=[
            vm((3, HEADS, HD, TOK), BF),
            vm((FEAT, WIDTH), BF),
            vm((TOK, WIDTH), BF),
            heads_of(3),
            heads_of(2),
            vm((2, HEADS, 1, TOK), jnp.int32),
            vm((HD, 8 * TOK), BF),
            vm((HD, keys), BF),
            vm((HD, keys), BF),
            vm((keys, HD), BF),
            vm((keys, HD), BF),
            vm((keys, TOK), F32),
            vm((1, 8 * TOK), F32),
            vm((keys, QTILE), F32),
            vm((TILES, keys, QTILE), BF),
            vm((TILES, keys, QTILE), BF),
            vm((TILES, 1, QTILE), F32),
            vm((WIDTH, FEAT), BF),
            vm((WIDTH, TOK), BF),
            heads_of(None),
            heads_of(None),
            heads_of(None),
            heads_of(None),
            vm((TILES, HD, QTILE), BF),
            heads_of(None),
            heads_of(2),
            heads_of(2),
            heads_of(2),
            vm((WIDTH, TOK), BF),
            vm((WIDTH, TOK), BF),
            heads_of(None),
            vm((4, 8, 8, TOK), F32),
            vm((2, nx, cx // 2, LANES), BF),
            vm((2, nx, cx // 2, LANES), BF),
            vm((2, cx // 2, LANES), F32),
            vm((nz, czp, LANES), BF),
            vm((nz, czp, LANES), BF),
            vm((HEADS, HALF_PAD, up(czp, 128)), BF),
            vm((HEADS, HALF_PAD, up(czp, 128)), BF),
            pltpu.SemaphoreType.DMA((6,)),
            pltpu.SemaphoreType.DMA((19, 8)),
            pltpu.SemaphoreType.DMA((19, 8)),
        ],
        compiler_params=pltpu.CompilerParams(
            collective_id=0, has_side_effects=True, vmem_limit_bytes=40 * 1024 * 1024),
        name="attention",
    )(q, k, v, w, target, lengths, segments)


def finish(grads, part, stats, dq_ref, dk_ref, dv_ref, wg_ref, loss_ref):
    slots = 16 * TOK
    packs = lax.axis_size("dp_0") * lax.axis_size("dp_1")
    lens = stats[1:2]
    ratio = jnp.float32(slots * 16 * packs) / lens
    loss_ref[...] = jnp.sum(stats[0:1] / (lens * (WIDTH / 16)), axis=1, keepdims=True)
    wg_ref[...] = part[...] * (ratio[:, 0:1] * (1.0 / slots))
    for j, ref in enumerate((dq_ref, dk_ref, dv_ref)):
        ref[...] = grads[j].reshape(FEAT, TOK).astype(F32) * ratio


def local(query_rows, key_rows, value_rows, out_weight, target, lengths, segments):
    stay = lambda value: pltpu.with_memory_space_constraint(value, pltpu.HBM)
    by_head = lambda rows: stay(rows[0].T.reshape(HEADS, HEAD_DIM, TOK))
    grads, part, stats = attention(
        by_head(query_rows), by_head(key_rows), by_head(value_rows), stay(out_weight),
        stay(target[0]), lengths, stay(segments))
    vmem = pl.BlockSpec(memory_space=pltpu.VMEM)
    dq, dk, dv, weight, loss = pl.pallas_call(
        finish,
        out_shape=[jax.ShapeDtypeStruct((FEAT, TOK), F32)] * 3 + [
            jax.ShapeDtypeStruct(part.shape, F32), jax.ShapeDtypeStruct((1, 1), F32)],
        in_specs=[vmem] * 3,
        out_specs=[vmem] * 5,
        compiler_params=pltpu.CompilerParams(vmem_limit_bytes=8 * 1024 * 1024),
        name="finish",
    )(grads, part, stats)
    return (dq.T[None], dk.T[None], dv.T[None], weight, loss.reshape(()))


def solution(mesh):
    torus = Mesh(mesh.devices.reshape(4, 8, 8, 2), ("dp_0", "dp_1", "patch_0", "patch_1"))
    return jax.shard_map(
        local,
        mesh=torus,
        in_specs=(P(DP, PATCH, None), P(DP, PATCH, None), P(DP, PATCH, None), P(),
                  P(DP, PATCH, None), P(DP), P(DP, PATCH)),
        out_specs=(P(DP, PATCH, None), P(DP, PATCH, None), P(DP, PATCH, None), P(PATCH, DP), P()),
        check_vma=False,
    )
```

```python
import math

import jax
import jax.numpy as jnp
from jax import lax
from jax.experimental import pallas as pl
from jax.experimental.pallas import tpu as pltpu
from jax.sharding import Mesh
from jax.sharding import PartitionSpec as P

WIDTH = 1152
HEADS = 8
HEAD_DIM = 72
FEAT = 576
TOK = 128
HALF = 36
HALF_PAD = 48
LANES = HEADS * HALF_PAD
PATCH = ("patch_0", "patch_1")
DP = ("dp_0", "dp_1")
DP_PATCH = ("dp_0", "dp_1", "patch_0", "patch_1")
NEG_LARGE = -1e30
MESH = pl.DeviceIdType.MESH
BF = jnp.bfloat16
F32 = jnp.float32
ORDER = (4, 3, 5, 2, 6, 1, 7)
QTILE = 256
TILES = 4
SLOTS = (0,) + ORDER
KCH = 256
CHUNKS = 8


def mm(a, b):
    return jnp.dot(a, b, preferred_element_type=F32)


def mmt(a, b):
    return lax.dot_general(a, b, (((1,), (1,)), ((), ())), preferred_element_type=F32)


def eye(n):
    r = lax.broadcasted_iota(jnp.int32, (n, n), 0)
    c = lax.broadcasted_iota(jnp.int32, (n, n), 1)
    return jnp.where(r == c, 1.0, 0.0).astype(BF)


def lanes(i, n):
    return pl.ds(pl.multiple_of(i * n, n), n)


def up(n, m):
    return (n + m - 1) // m * m


def kernel(
    q_hbm, k_hbm, v_hbm, w_hbm, tgt_hbm, len_ref, seg_hbm,
    grad_rx, wg_ref, stat_ref,
    snd, w_ref, tgt_ref, rx, sib, segs, qt, kt, vt, km, vm, gk, gq, top_ref, s_ref, p_ref,
    ds_ref, w_tr, tgt_tr, attn_snd, attn_rx, go_snd, go_rx, gos, dq_acc, q_snd, xs_snd, xs_rx,
    own_kv, kv_snd,
    gt, gt_sib, attn_sib, stats, x_snd, x_rx, x_sum, z_snd, z_rx, y_snd, y_rx,
    lsem, ssem, rsem, rslot,
):
    x = lax.axis_index("dp_0")
    z = lax.axis_index("dp_1")
    y = lax.axis_index("patch_0")
    c = lax.axis_index("patch_1")
    nx = lax.axis_size("dp_0")
    nz = lax.axis_size("dp_1")
    HD = HEAD_DIM
    chip = lambda d: lax.rem(y + d, 8)
    at = lambda h: {"patch_0": h}
    back = lambda d: SLOTS.index((8 - d) % 8)
    xs = [(lax.rem(x + d, nx)) for d in range(1, nx)]
    zs = [(lax.rem(z + d, nz)) for d in range(1, nz)]
    sibling = {"patch_1": 1 - c}
    barrier = pltpu.get_barrier_semaphore()
    for d in range(1, 8):
        pl.semaphore_signal(barrier, inc=1, device_id=at(chip(d)), device_id_type=MESH)
    pl.semaphore_signal(barrier, inc=1, device_id=sibling, device_id_type=MESH)
    for o in xs:
        pl.semaphore_signal(barrier, inc=1, device_id={"dp_0": o}, device_id_type=MESH)
    for o in zs:
        pl.semaphore_signal(barrier, inc=1, device_id={"dp_1": o}, device_id_type=MESH)

    loads = [
        pltpu.make_async_copy(src, dst, lsem.at[i])
        for i, (src, dst) in enumerate((
            (q_hbm, snd.at[0]), (k_hbm, snd.at[1]), (v_hbm, snd.at[2]), (seg_hbm, segs.at[0, 0]),
            (w_hbm, w_ref), (tgt_hbm, tgt_ref)))
    ]
    for load in loads:
        load.start()

    def send(kind, src, dst, to, slot=None):
        return pltpu.make_async_remote_copy(
            src_ref=src, dst_ref=dst, send_sem=ssem.at[kind],
            recv_sem=rsem.at[kind] if slot is None else rslot.at[slot],
            device_id=to, device_id_type=MESH)

    for load in loads[:4]:
        load.wait()
    pl.semaphore_wait(barrier, 8 + len(xs) + len(zs))
    for d in ORDER:
        send(1, segs.at[0, 0], segs.at[0, back(d)], at(chip(d))).start()
    for d in ORDER:
        h = chip(d)
        send(0, snd.at[:, h], rx.at[back(d)], at(h), back(d)).start()
    send(2, snd.at[1:3, y], sib.at[0], sibling, 8).start()

    id256 = eye(256)
    id128 = eye(128)
    loads[4].wait()
    loads[5].wait()
    for j in range(5):
        n = 256 if j < 4 else 128
        cols = slice(256 * j, 256 * j + n)
        unit = id256 if n == 256 else id128
        w_tr[cols, :] = mmt(unit, w_ref[:, cols]).astype(BF)
        tgt_tr[cols, :] = mmt(unit, tgt_ref[:, cols]).astype(BF)
    length = len_ref[0]
    vt[HD:HD + 8, :] = jnp.ones((8, 16 * TOK), BF)
    top_ref[...] = jnp.full((8, 8 * TOK), NEG_LARGE, F32)

    def groups(parity, i):
        number = 2 * chip(SLOTS[i]) + (c if parity == 0 else 1 - c)
        at_pos = number * TOK + lax.broadcasted_iota(jnp.int32, (1, TOK), 1)
        group = jnp.where(at_pos < length, segs[parity, i], -1).astype(F32)
        row = (8 * parity + i) * TOK
        gk[row:row + TOK, :] = mmt(id128, jnp.broadcast_to(group, (TOK, TOK)).astype(BF))
        if parity == 0:
            gq[:, i * TOK:(i + 1) * TOK] = group

    def place(block, kb, vb):
        part = slice(block * TOK, (block + 1) * TOK)
        kt[:, part] = kb
        vt[0:HD, part] = vb
        km[part, :] = mmt(id128, kb).astype(BF)
        vm[part, :] = mmt(id128, vb).astype(BF)

    def running(v, op, into):
        for i in range(v.shape[0] // 8):
            into = op(into, v[8 * i:8 * i + 8])
        return into

    def score(block, q0, q1):
        part = slice(block * TOK, (block + 1) * TOK)
        sc = mm(km[part, :], qt[:, q0 * TOK:q1 * TOK])
        g = gk[part, :]
        for qb in range(q0, q1):
            cols = slice(qb * TOK, (qb + 1) * TOK)
            sub = jnp.where(g == gq[:, cols], sc[:, (qb - q0) * TOK:(qb - q0 + 1) * TOK], NEG_LARGE)
            s_ref[part, cols] = sub
            top_ref[:, cols] = running(sub, jnp.maximum, top_ref[:, cols])

    def place_own(i, qb, kb, vb):
        qt[:, i * TOK:(i + 1) * TOK] = qb
        place(i, kb, vb)
        if i:
            score(i, 0, i)
        for block in list(range(i + 1)) + [8 + j for j in range(i - 1)]:
            score(block, i, i + 1)

    def place_sibling(i, upto):
        send(2, rx.at[i, 1:3], sib.at[i], sibling, 8 + i).wait_recv()
        place(8 + i, sib[i, 0], sib[i, 1])
        for q0 in range(0, upto, 2):
            score(8 + i, q0, min(q0 + 2, upto))

    send(1, segs.at[0, 0:7], segs.at[0, 1:8], at(y)).wait_recv()
    send(3, segs.at[0], segs.at[1], sibling).start()
    for i in range(8):
        groups(0, i)
    place_own(0, snd[0, y], snd[1, y], snd[2, y])
    send(3, segs.at[0], segs.at[1], sibling).wait_recv()
    for i in range(8):
        groups(1, i)
    for i in range(1, 8):
        send(0, snd.at[:, y], rx.at[i], at(y), i).wait_recv()
        send(2, rx.at[i, 1:3], sib.at[i], sibling, 8 + i).start()
        place_own(i, rx[i, 0], rx[i, 1], rx[i, 2])
        place_sibling(i - 1, i + 1)
    place_sibling(7, 8)

    scale = 1.0 / math.sqrt(HEAD_DIM)
    to_two = scale / math.log(2.0)
    rdens = []
    for t in range(TILES):
        cols = slice(t * QTILE, (t + 1) * QTILE)
        top = jnp.max(top_ref[:, cols], axis=0, keepdims=True)
        for i in range(2 * CHUNKS):
            part = slice(i * TOK, (i + 1) * TOK)
            p_ref[part, cols] = jnp.exp2((s_ref[part, cols] - top) * to_two).astype(BF)
        sums = mm(vt[...], p_ref[:, cols])
        inv = 1.0 / sums[HD:HD + 1]
        rdens.append(inv)
        out = (sums[0:HD] * inv).astype(BF)
        for half in range(2):
            i = 2 * t + half
            attn_snd[i] = out[:, half * TOK:(half + 1) * TOK]
            if i:
                send(4, attn_snd.at[i], attn_rx.at[y], at(chip(SLOTS[i]))).start()

    attn_rx[y] = attn_snd[0]
    send(4, attn_snd.at[0:7], attn_rx.at[0:7], at(y)).wait_recv()

    send(10, attn_rx, attn_sib, sibling).start()
    attn_t = attn_rx[...].reshape(FEAT, TOK)
    position = (2 * y + c) * TOK + lax.broadcasted_iota(jnp.int32, (1, TOK), 1)
    live = position < length
    out_t = mm(w_tr[...], attn_t)
    error = jnp.where(live, out_t - tgt_tr[...].astype(F32), 0.0)
    grad_t = (2.0 * error).astype(BF)
    gt[...] = grad_t
    squares = running(error * error, jnp.add, jnp.zeros((8, TOK), F32))
    squares = jnp.sum(squares, axis=0, keepdims=True)
    lens = jnp.full((1, TOK), length.astype(F32), F32)
    row = lax.broadcasted_iota(jnp.int32, (8, TOK), 0)
    stats[0, 0] = jnp.where(row == 0, squares, jnp.where(row == 1, lens, 0.0))
    send(9, gt, gt_sib, sibling).start()
    send(11, stats.at[0, 0], stats.at[0, 1], sibling).start()
    go_snd[...] = mm(w_ref[...], grad_t).astype(BF).reshape(HEADS, HD, TOK)
    for d in ORDER:
        h = chip(d)
        send(5, go_snd.at[h], go_rx.at[back(d)], at(h)).start()
    go_rx[0] = go_snd[y]

    parts = []
    for h in range(HEADS):
        r = lax.broadcasted_iota(jnp.int32, (HALF_PAD, FEAT), 0)
        f = lax.broadcasted_iota(jnp.int32, (HALF_PAD, FEAT), 1)
        hit = jnp.logical_and(f - r == HD * h + HALF * c, r < HALF)
        parts.append(jnp.where(hit, 1.0, 0.0).astype(BF))
    pick = jnp.concatenate(parts, axis=0)
    send(10, attn_rx, attn_sib, sibling).wait_recv()
    attn_both = jnp.concatenate(
        [mm(pick, attn_t), mm(pick, attn_sib[...].reshape(FEAT, TOK))], axis=1).astype(BF)
    send(9, gt, gt_sib, sibling).wait_recv()
    send(11, stats.at[0, 0], stats.at[0, 1], sibling).wait_recv()
    stats[1, x] = stats[0, 0] + stats[0, 1]
    cx = WIDTH // nx
    cz = cx // nz
    czp = up(cz, 8)
    ch = cx // 2
    for half in range(2):
        for o in xs + [x]:
            rows = pl.ds(pl.multiple_of(o * cx + half * ch, 16), ch)
            both = jnp.concatenate([gt[rows, :], gt_sib[rows, :]], axis=1)
            x_snd[half, o] = mmt(both, attn_both).astype(BF)
            if o is not x:
                send(12 + half, x_snd.at[half, o], x_rx.at[half, x], {"dp_0": o}).start()
                if half == 0:
                    send(18, stats.at[1, x], stats.at[1, x], {"dp_0": o}).start()

    def sum_over_x(half):
        if nx > 1:
            send(12 + half, x_snd.at[half, 0:nx - 1], x_rx.at[half, 0:nx - 1], at(y)).wait_recv()
        acc = x_snd[half, x].astype(F32)
        for o in xs:
            acc = acc + x_rx[half, o].astype(F32)
        x_sum[half] = acc
        for k in range(nz // 2):
            to = half * (nz // 2) + k
            z_snd[to, 0:cz] = x_sum[half, k * cz:(k + 1) * cz, :].astype(BF)
            if czp > cz:
                z_snd[to, cz:czp] = jnp.zeros((czp - cz, LANES), BF)

            @pl.when(to != z)
            def _():
                send(14, z_snd.at[to], z_rx.at[z], {"dp_1": to}).start()

    send(5, go_snd.at[0:7], go_rx.at[1:8], at(y)).wait_recv()
    deltas = []
    for t in range(TILES):
        both = jnp.concatenate([go_rx[2 * t], go_rx[2 * t + 1]], axis=1).astype(F32)
        scaled = (both * rdens[t]).astype(BF)
        gos[:, t * QTILE:(t + 1) * QTILE] = scaled
        attn = jnp.concatenate([attn_snd[2 * t], attn_snd[2 * t + 1]], axis=1)
        deltas.append(jnp.sum(scaled.astype(F32) * attn.astype(F32), axis=0, keepdims=True))

    def backward(i, slot, first):
        part = slice(i * KCH, (i + 1) * KCH)
        for t in range(TILES):
            cols = slice(t * QTILE, (t + 1) * QTILE)
            dp = mm(vm[part, :], gos[:, cols])
            ds_ref[slot, :, cols] = (p_ref[part, cols].astype(F32) * (dp - deltas[t])).astype(BF)
        dv = mmt(gos[...], p_ref[part, :])
        dk = mmt(qt[...], ds_ref[slot]) * scale
        dq = mm(kt[:, part], ds_ref[slot])
        dq_acc[...] = dq if first else dq_acc[...] + dq
        return dk, dv

    def hand_over(j):
        send(7, xs_snd.at[j], xs_rx.at[j], sibling, 16 + j).wait_recv()
        for half in range(2):
            i = 2 * j + half
            cols = slice(half * TOK, (half + 1) * TOK)
            for g in range(2):
                kv_snd[g, i] = (own_kv[j, g, :, cols] + xs_rx[j, g, :, cols].astype(F32)).astype(BF)
            if i:
                send(8, kv_snd.at[:, i], grad_rx.at[1:3, y], at(chip(SLOTS[i]))).start()

    for j in range(4):
        dk, dv = backward(j + 4, 0, j == 0)
        xs_snd[j, 0] = dk.astype(BF)
        xs_snd[j, 1] = dv.astype(BF)
        send(7, xs_snd.at[j], xs_rx.at[j], sibling, 16 + j).start()
        dk, dv = backward(j, 1, False)
        own_kv[j, 0] = dk
        own_kv[j, 1] = dv
        if j:
            hand_over(j - 1)
    dq = (dq_acc[...] * scale).astype(BF)
    for i in range(8):
        q_snd[i] = dq[:, i * TOK:(i + 1) * TOK]
        if i:
            send(6, q_snd.at[i], grad_rx.at[0, y], at(chip(SLOTS[i]))).start()
    hand_over(3)
    grad_rx[0, y] = q_snd[0]
    grad_rx[1, y] = kv_snd[0, 0]
    grad_rx[2, y] = kv_snd[1, 0]

    sum_over_x(0)
    tot = stats[1, x]
    if nx > 1:
        send(18, stats.at[1, 0:nx - 1], stats.at[1, 0:nx - 1], at(y)).wait_recv()
    for o in xs:
        tot = tot + stats[1, o]
    stats[2, z] = tot
    for o in zs:
        send(15, stats.at[2, z], stats.at[2, z], {"dp_1": o}).start()
    sum_over_x(1)

    send(14, z_snd.at[0:nz - 1], z_rx.at[0:nz - 1], at(y)).wait_recv()
    send(15, stats.at[2, 0:nz - 1], stats.at[2, 0:nz - 1], at(y)).wait_recv()
    acc = z_snd[z].astype(F32)
    tot = stats[2, z]
    for o in zs:
        acc = acc + z_rx[o].astype(F32)
        tot = tot + stats[2, o]
    stats[3, y] = tot
    turned = mmt(eye(LANES), acc.astype(BF)).astype(BF)
    y_snd[:, :, 0:czp] = turned.reshape(HEADS, HALF_PAD, czp)
    for d in ORDER:
        h = chip(d)
        send(16, y_snd.at[h], y_rx.at[y], at(h)).start()
        send(17, stats.at[3, y], stats.at[3, y], at(h)).start()
    y_rx[y] = y_snd[y]
    send(6, q_snd.at[0:7], grad_rx.at[0, 0:7], at(y)).wait_recv()
    send(8, kv_snd.at[:, 0:7], grad_rx.at[1:3, 0:7], at(y)).wait_recv()
    send(16, y_snd.at[0:7], y_rx.at[0:7], at(y)).wait_recv()
    send(17, stats.at[3, 0:7], stats.at[3, 0:7], at(y)).wait_recv()
    tot = jnp.zeros((8, TOK), F32)
    acc = jnp.zeros((HALF_PAD, czp), F32)
    for s in range(8):
        tot = tot + stats[3, s]
        acc = acc + y_rx[s, :, 0:czp].astype(F32)
    stat_ref[...] = tot
    wg_ref[...] = acc[0:HALF, 0:cz]

    send(0, rx.at[0:7], rx.at[0:7], at(y), 0).wait_send()
    send(1, segs.at[0, 0:7], segs.at[0, 0:7], at(y)).wait_send()
    send(2, sib, sib, sibling, 8).wait_send()
    send(3, segs.at[0], segs.at[1], sibling).wait_send()
    send(4, attn_snd.at[0:7], attn_rx.at[0:7], at(y)).wait_send()
    send(5, go_snd.at[0:7], go_rx.at[1:8], at(y)).wait_send()
    send(6, q_snd.at[0:7], grad_rx.at[0, 0:7], at(y)).wait_send()
    send(7, xs_snd, xs_rx, sibling, 16).wait_send()
    send(8, kv_snd.at[:, 0:7], grad_rx.at[1:3, 0:7], at(y)).wait_send()
    send(9, gt, gt_sib, sibling).wait_send()
    send(10, attn_rx, attn_sib, sibling).wait_send()
    send(11, stats.at[0, 0], stats.at[0, 1], sibling).wait_send()
    if nx > 1:
        for half in range(2):
            send(12 + half, x_snd.at[half, 0:nx - 1], x_rx.at[half, 0:nx - 1], at(y)).wait_send()
        send(18, stats.at[1, 0:nx - 1], stats.at[1, 0:nx - 1], at(y)).wait_send()
    send(14, z_snd.at[0:nz - 1], z_rx.at[0:nz - 1], at(y)).wait_send()
    send(15, stats.at[2, 0:nz - 1], stats.at[2, 0:nz - 1], at(y)).wait_send()
    send(16, y_snd.at[0:7], y_rx.at[0:7], at(y)).wait_send()
    send(17, stats.at[3, 0:7], stats.at[3, 0:7], at(y)).wait_send()


def attention(q, k, v, w, target, lengths, segments):
    vm = pltpu.VMEM
    vmem = pl.BlockSpec(memory_space=pltpu.VMEM)
    hbm = pl.BlockSpec(memory_space=pltpu.HBM)
    keys = 16 * TOK
    nx = lax.axis_size("dp_0")
    nz = lax.axis_size("dp_1")
    cx = WIDTH // nx
    cz = cx // nz
    czp = up(cz, 8)
    HD = HEAD_DIM
    heads_of = lambda n: vm((HEADS, HD, TOK) if n is None else (HEADS, n, HD, TOK), BF)
    return pl.pallas_call(
        kernel,
        out_shape=[
            jax.ShapeDtypeStruct((3, HEADS, HD, TOK), BF),
            jax.ShapeDtypeStruct((HALF, cz), F32),
            jax.ShapeDtypeStruct((8, TOK), F32),
        ],
        in_specs=[hbm] * 5 + [pl.BlockSpec(memory_space=pltpu.SMEM), hbm],
        out_specs=[vmem] * 3,
        scratch_shapes=[
            vm((3, HEADS, HD, TOK), BF),
            vm((FEAT, WIDTH), BF),
            vm((TOK, WIDTH), BF),
            heads_of(3),
            heads_of(2),
            vm((2, HEADS, 1, TOK), jnp.int32),
            vm((HD, 8 * TOK), BF),
            vm((HD, keys), BF),
            vm((HD + 8, keys), BF),
            vm((keys, HD), BF),
            vm((keys, HD), BF),
            vm((keys, TOK), F32),
            vm((1, 8 * TOK), F32),
            vm((8, 8 * TOK), F32),
            vm((keys, 8 * TOK), F32),
            vm((keys, 8 * TOK), BF),
            vm((2, KCH, 8 * TOK), BF),
            vm((WIDTH, FEAT), BF),
            vm((WIDTH, TOK), BF),
            heads_of(None),
            heads_of(None),
            heads_of(None),
            heads_of(None),
            vm((HD, 8 * TOK), BF),
            vm((HD, 8 * TOK), F32),
            heads_of(None),
            vm((4, 2, HD, KCH), BF),
            vm((4, 2, HD, KCH), BF),
            vm((4, 2, HD, KCH), F32),
            vm((2, HEADS, HD, TOK), BF),
            vm((WIDTH, TOK), BF),
            vm((WIDTH, TOK), BF),
            heads_of(None),
            vm((4, 8, 8, TOK), F32),
            vm((2, nx, cx // 2, LANES), BF),
            vm((2, nx, cx // 2, LANES), BF),
            vm((2, cx // 2, LANES), F32),
            vm((nz, czp, LANES), BF),
            vm((nz, czp, LANES), BF),
            vm((HEADS, HALF_PAD, up(czp, 128)), BF),
            vm((HEADS, HALF_PAD, up(czp, 128)), BF),
            pltpu.SemaphoreType.DMA((6,)),
            pltpu.SemaphoreType.DMA((19,)),
            pltpu.SemaphoreType.DMA((19,)),
            pltpu.SemaphoreType.DMA((20,)),
        ],
        compiler_params=pltpu.CompilerParams(
            collective_id=0, has_side_effects=True, vmem_limit_bytes=40 * 1024 * 1024),
        name="attention",
    )(q, k, v, w, target, lengths, segments)


def finish(grads, part, stats, dq_ref, dk_ref, dv_ref, wg_ref, loss_ref):
    slots = 16 * TOK
    packs = lax.axis_size("dp_0") * lax.axis_size("dp_1")
    lens = stats[1:2]
    ratio = jnp.float32(slots * 16 * packs) / lens
    loss_ref[...] = jnp.sum(stats[0:1] / (lens * (WIDTH / 16)), axis=1, keepdims=True)
    wg_ref[...] = part[...] * (ratio[:, 0:1] * (1.0 / slots))
    for j, ref in enumerate((dq_ref, dk_ref, dv_ref)):
        ref[...] = grads[j].reshape(FEAT, TOK).astype(F32) * ratio


def local(query_rows, key_rows, value_rows, out_weight, target, lengths, segments):
    stay = lambda value: pltpu.with_memory_space_constraint(value, pltpu.HBM)
    by_head = lambda rows: stay(rows[0].T.reshape(HEADS, HEAD_DIM, TOK))
    grads, part, stats = attention(
        by_head(query_rows), by_head(key_rows), by_head(value_rows), stay(out_weight),
        stay(target[0]), lengths, stay(segments))
    vmem = pl.BlockSpec(memory_space=pltpu.VMEM)
    dq, dk, dv, weight, loss = pl.pallas_call(
        finish,
        out_shape=[jax.ShapeDtypeStruct((FEAT, TOK), F32)] * 3 + [
            jax.ShapeDtypeStruct(part.shape, F32), jax.ShapeDtypeStruct((1, 1), F32)],
        in_specs=[vmem] * 3,
        out_specs=[vmem] * 5,
        compiler_params=pltpu.CompilerParams(vmem_limit_bytes=8 * 1024 * 1024),
        name="finish",
    )(grads, part, stats)
    return (dq.T[None], dk.T[None], dv.T[None], weight, loss.reshape(()))


def solution(mesh):
    torus = Mesh(mesh.devices.reshape(4, 8, 8, 2), ("dp_0", "dp_1", "patch_0", "patch_1"))
    return jax.shard_map(
        local,
        mesh=torus,
        in_specs=(P(DP, PATCH, None), P(DP, PATCH, None), P(DP, PATCH, None), P(),
                  P(DP, PATCH, None), P(DP), P(DP, PATCH)),
        out_specs=(P(DP, PATCH, None), P(DP, PATCH, None), P(DP, PATCH, None), P(PATCH, DP), P()),
        check_vma=False,
    )
```
